256 devices in a mesh: dp: 32 (over z, x), heads: 8 (over y, core).
Axes of the slice: x: 4, y: 4, z: 8, core: 2. Of those that a mesh axis runs over, the one named last changes fastest.
Arguments:
- queries: bfloat16 [256, 16, 128], P('dp', 'heads'), may hold values from -12 to 12
- key_cache: bfloat16 [2048, 8, 256, 128], P('dp', 'heads'), may hold values from -6 to 6
- value_cache: bfloat16 [2048, 8, 256, 128], P('dp', 'heads'), may hold values from -6 to 6
- lengths_seen: int32 [256, 8], P('dp', 'heads'), may hold values from 1025 to 2048, as said below
- page_table: int32 [256, 8], P('dp'), may hold values from 0 to 63, as said below
- finished: int32 [256], P('dp'), may hold values from 0 to 1, as said below
- move_plan: int32 [1024, 3], P('dp'), may hold values from 0 to 63, as said below
Outputs:
- attention: bfloat16 [256, 16, 128], P('dp', 'heads')
The draws below stay inside these ranges and needn't reach their ends.
Inputs may be any that keep to these rules, and one draw needn't show every extreme that they name: `lengths_seen`: each session's length, the largest entry of its row, lies between (5) * 256 + 1 and 2048. `page_table`: the 8 rows of one device's sessions hold each of that device's slot numbers exactly once. At most 2 sessions of one device are finished. `move_plan`: A row's source device differs from its receiving device; the destination slots of one receiving device are distinct, and each holds, after the moves, a page below the length of a session that is not finished. One device receives at most 2 pages from one source device, and on every device some source sends exactly 2.
All inputs are finite; a program needn't handle non-finite values.
Results may differ from the reference program's by a relative error of at most 0.008.
Values may be sent and summed in bfloat16 or wider, within the bound.
A program may use at most 64 MiB of HBM per device.

```python
import jax
import jax.numpy as jnp
from jax import lax

HD = 128
QH = 16
KVH = 8
PAGE = 256
PAGES_MAX = 8
MOVES_DEV = 32
SESS_DEV = 8
SLOTS = 64
SESSIONS = 256
N_DP = 32
N_HEADS = 8


def joint_layout(key):
    base = jax.random.fold_in(key, 911)
    subkeys = jax.random.split(base, 9)
    device_ids = jnp.arange(N_DP, dtype=jnp.int32)
    true_length = jax.random.randint(subkeys[0], (N_DP, SESS_DEV), (PAGES_MAX - 3) * PAGE + 1, PAGES_MAX * PAGE + 1, dtype=jnp.int32)
    holder = jax.random.randint(subkeys[1], (N_DP, SESS_DEV, 1), 0, N_HEADS, dtype=jnp.int32)
    shortfall = jax.random.randint(subkeys[2], (N_DP, SESS_DEV, N_HEADS), 1, PAGE + 1, dtype=jnp.int32)
    columns = lax.broadcasted_iota(jnp.int32, (N_DP, SESS_DEV, N_HEADS), 2)
    seen = jnp.where(columns == holder, true_length[:, :, None], true_length[:, :, None] - shortfall)
    tables = jax.vmap(lambda sub: jax.random.permutation(sub, SLOTS))(jax.random.split(subkeys[3], N_DP)).astype(jnp.int32)
    order = jax.vmap(lambda sub: jax.random.permutation(sub, SESS_DEV))(jax.random.split(subkeys[4], N_DP)).astype(jnp.int32)
    coins = jax.random.randint(subkeys[5], (N_DP, SESS_DEV), 0, 2, dtype=jnp.int32)
    finished = jnp.where(order < SESS_DEV // 3, coins, 0).astype(jnp.int32)
    used_pages = (true_length + PAGE - 1) // PAGE
    page_index = lax.broadcasted_iota(jnp.int32, (N_DP, SESS_DEV, PAGES_MAX), 2)
    eligible = (page_index < used_pages[:, :, None]) & (finished[:, :, None] == 0)
    ranking = jax.vmap(lambda sub: jax.random.permutation(sub, SLOTS))(jax.random.split(subkeys[6], N_DP)).astype(jnp.int32)
    priority = eligible.reshape(N_DP, SLOTS).astype(jnp.int32) * SLOTS + ranking
    chosen = lax.top_k(priority, MOVES_DEV)[1].astype(jnp.int32)
    target = jnp.take_along_axis(tables, chosen, axis=1)
    offsets = jax.vmap(lambda sub: jax.random.permutation(sub, N_DP - 1))(jax.random.split(subkeys[7], N_DP)).astype(jnp.int32) + 1
    rows = jnp.arange(MOVES_DEV, dtype=jnp.int32)
    offset_index = rows % (N_DP - 1)
    source_device = (device_ids[:, None] + offsets[:, offset_index]) % N_DP
    source_slot = jax.random.randint(subkeys[8], (N_DP, MOVES_DEV), 0, SLOTS, dtype=jnp.int32)
    plan = jnp.stack([source_device, source_slot, target], axis=2).reshape(N_DP * MOVES_DEV, 3).astype(jnp.int32)
    return (seen.reshape(SESSIONS, N_HEADS), tables.reshape(SESSIONS, PAGES_MAX), finished.reshape(SESSIONS), plan)


def draw_lengths_seen(key, part):
    return joint_layout(key)[0]


def draw_page_table(key, part):
    return joint_layout(key)[1]


def draw_finished(key, part):
    return joint_layout(key)[2]


def draw_move_plan(key, part):
    return joint_layout(key)[3]


def shard_levels(own_key, extent, cuts, least, high):
    def one(position, parts):
        draws = jax.random.uniform(jax.random.fold_in(jax.random.fold_in(own_key, 6), position), (parts,), jnp.float32, least / len(cuts), high / len(cuts))
        return jnp.repeat(jnp.exp(draws), extent[position] // parts).reshape((-1,) + (1,) * (len(extent) - position - 1))

    factor_of = one(*cuts[0])
    for cut in cuts[1:]:
        factor_of = factor_of * one(*cut)
    return factor_of


def normal_values(rng, extent, deviation, most, cuts=(), kind=jnp.bfloat16):
    gain = shard_levels(rng, extent, cuts, -0.22, 0.18) if cuts else 1.0
    result = jax.random.normal(rng, extent, jnp.float32) * deviation * gain
    return jnp.minimum(jnp.maximum(result, -most), most).astype(kind)


def setup_inputs(seed: int = 0) -> dict:
    streams_of = jax.random.split(jax.random.key(seed), 8)
    queries = normal_values(streams_of[0], (SESSIONS, QH, HD), 2.0, 12.0, ((0, 32), (1, 8)))
    key_cache = normal_values(streams_of[1], (N_DP * SLOTS, KVH, PAGE, HD), 1.0, 6.0, ((0, 32), (1, 8)))
    value_cache = normal_values(streams_of[2], (N_DP * SLOTS, KVH, PAGE, HD), 1.0, 6.0, ((0, 32), (1, 8)))
    lengths_seen = draw_lengths_seen(jax.random.fold_in(streams_of[7], 71), 0)
    page_table = draw_page_table(jax.random.fold_in(streams_of[7], 71), 0)
    finished = draw_finished(jax.random.fold_in(streams_of[7], 71), 0)
    move_plan = draw_move_plan(jax.random.fold_in(streams_of[7], 71), 0)
    return dict(queries=queries, key_cache=key_cache, value_cache=value_cache, lengths_seen=lengths_seen, page_table=page_table, finished=finished, move_plan=move_plan)


softcap_limit = 50.0
score_divisor = 12.0


def reference(queries, key_cache, value_cache, lengths_seen, page_table, finished, move_plan):
    key_pages = key_cache.reshape(N_DP, SLOTS, KVH, PAGE, HD)
    value_pages = value_cache.reshape(N_DP, SLOTS, KVH, PAGE, HD)
    receiver = (jnp.arange(N_DP * MOVES_DEV, dtype=jnp.int32) // MOVES_DEV).astype(jnp.int32)
    source_device = move_plan[:, 0]
    source_slot = move_plan[:, 1]
    target_slot = move_plan[:, 2]
    key_pages = key_pages.at[receiver, target_slot].set(key_pages[source_device, source_slot])
    value_pages = value_pages.at[receiver, target_slot].set(value_pages[source_device, source_slot])
    length = jnp.max(lengths_seen, axis=1)
    home = (jnp.arange(SESSIONS, dtype=jnp.int32) // SESS_DEV).astype(jnp.int32)
    group_size = QH // KVH

    def attend_session(inputs):
        query_row, slot_row, device, session_length, is_finished = inputs
        picked_keys = key_pages[device, slot_row]
        picked_values = value_pages[device, slot_row]
        token_keys = picked_keys.transpose(1, 0, 2, 3).reshape(KVH, PAGES_MAX * PAGE, HD).astype(jnp.float32)
        token_values = picked_values.transpose(1, 0, 2, 3).reshape(KVH, PAGES_MAX * PAGE, HD).astype(jnp.float32)
        grouped = query_row.reshape(KVH, group_size, HD).astype(jnp.float32)
        raw_scores = jnp.einsum('kgd,ktd->kgt', grouped, token_keys, precision=lax.Precision.HIGHEST) / score_divisor
        capped = softcap_limit * jnp.tanh(raw_scores / softcap_limit)
        places = lax.broadcasted_iota(jnp.int32, capped.shape, 2)
        weights = jnp.where(places < session_length, jnp.exp(capped), jnp.float32(0.0)).astype(jnp.bfloat16)
        weights = lax.optimization_barrier(weights).astype(jnp.float32)
        numerator = jnp.einsum('kgt,ktd->kgd', weights, token_values, precision=lax.Precision.HIGHEST)
        denominator = jnp.sum(weights, axis=2)
        output = (numerator / denominator[:, :, None]).reshape(QH, HD)
        return jnp.where(is_finished == 1, jnp.float32(0.0), output).astype(jnp.bfloat16)

    return lax.map(attend_session, (queries, page_table, home, length, finished))
```

```python
import functools

import jax
import jax.numpy as jnp
from jax import lax
from jax.experimental import pallas as pl
from jax.experimental.pallas import tpu as pltpu
from jax.sharding import PartitionSpec as P

NZ, NX = 8, 4
MESH = pl.DeviceIdType.MESH
F32, BF16, I32 = jnp.float32, jnp.bfloat16, jnp.int32


def hops(o):
    z, x = o // NX, o % NX
    return min(z, NZ - z) + min(x, NX - x)


def opposite(o):
    z, x = o // NX, o % NX
    return ((NZ - z) % NZ) * NX + (NX - x) % NX


NEAR_FIRST = sorted(range(1, NZ * NX), key=hops)
FAR_FIRST = NEAR_FIRST[::-1]


def nt(a, b, precision=None):
    return lax.dot_general(
        a, b, (((1,), (1,)), ((), ())), precision=precision, preferred_element_type=F32
    )


def nn(a, b, precision=None):
    return lax.dot_general(
        a, b, (((1,), (0,)), ((), ())), precision=precision, preferred_element_type=F32
    )


def iota(shape, dim):
    return lax.broadcasted_iota(I32, shape, dim)


def kernel(
    n_dp, n_heads,
    table_s, q_ref, k_hbm, v_hbm, seen_ref, table_ref, fin_ref, plan_ref,
    out_ref,
    k_buf, v_buf, ask_q, ask_w, got_q, got_w, len_out, len_in, len_max, got_len,
    e_loc, e_far, give, back,
    kv_sem, h_send, h_recv, q_send, q_recv, w_send, w_recv, l_send, l_recv, b_send, b_recv,
):
    me, head = lax.axis_index("dp"), lax.axis_index("heads")
    mz, mx = me // NX, lax.rem(me, NX)

    def peer(o):
        z, x = o // NX, o % NX
        return lax.rem(mz + z, NZ) * NX + lax.rem(mx + x, NX)

    def across(k):
        return lax.rem(head + k, n_heads)

    barrier = pltpu.get_barrier_semaphore()
    for o in FAR_FIRST:
        pl.semaphore_signal(barrier, inc=1, device_id={"dp": peer(o)}, device_id_type=MESH)
    for k in range(1, n_heads):
        pl.semaphore_signal(barrier, inc=1, device_id={"heads": across(k)}, device_id_type=MESH)

    k_copy = pltpu.make_async_copy(k_hbm, k_buf, kv_sem.at[0])
    v_copy = pltpu.make_async_copy(v_hbm, v_buf, kv_sem.at[1])
    k_copy.start()
    v_copy.start()

    src, slot, dest = plan_ref[0:1, :], plan_ref[1:2, :], plan_ref[2:3, :]
    rows = src.shape[1]
    off = ((src // NX - mz + NZ) % NZ) * NX + (src % NX - mx + NX) % NX
    sub, lane = iota((rows, rows), 0), iota((rows, rows), 1)
    off_f = off.astype(F32)
    off_col = jnp.sum(jnp.where(sub == lane, off_f, 0.0), axis=1, keepdims=True)
    same = (off_col == off_f) & (sub < lane)
    rank = jnp.sum(jnp.where(same, 1.0, 0.0), axis=0, keepdims=True)
    place = off_f * 2.0 + rank
    sub8 = iota((8, rows), 0)
    entry = jnp.zeros((8, rows), F32)
    for t in range(8):
        hit = table_ref[:, t : t + 1] == dest
        entry = entry + jnp.where(hit, (sub8 * 8 + t).astype(F32), 0.0)
    entry = jnp.sum(entry, axis=0, keepdims=True)
    session = jnp.floor(entry * 0.125)
    page = entry - session * 8.0

    hot16 = jnp.where((iota((16, rows), 0) // 2).astype(F32) == session, 1.0, 0.0).astype(BF16)
    n_back = n_dp * 8
    r8 = iota((n_back, rows), 0)
    lies = (r8 // 8 * 2 + (r8 % 8 // 2) % 2).astype(F32) == place
    spread = jnp.where(lies, 1.0, 0.0).astype(BF16)
    pick = nt(spread, hot16)
    row_a, col_a = iota((n_back, 16), 0), iota((n_back, 16), 1)
    pick = jnp.where((row_a % 2 == col_a % 2) & (row_a % 8 < 4), pick, 0.0).astype(BF16)
    q16 = q_ref[...].astype(F32).reshape(16, 128).astype(BF16)
    ask_q[...] = nn(pick, q16).reshape(n_dp, 8, 128).astype(BF16)
    word = slot.astype(F32) + 64.0 * session + 512.0 * page
    at = iota((n_dp, rows), 0).astype(F32) == off_f
    word_t = jnp.where(iota((128, rows), 0).astype(F32) == rank, word, 0.0)
    words = nt(jnp.where(at, 1.0, 0.0), word_t, lax.Precision.HIGHEST)
    ask_w[...] = words.astype(I32).reshape(n_dp, 1, 128)

    take = nt(hot16, spread)
    row_b, col_b = iota((16, n_back), 0), iota((16, n_back), 1)
    fits = row_b % 2 == col_b % 2
    take_num = jnp.where(fits & (col_b % 8 < 4), take, 0.0).astype(BF16)
    take_den = jnp.where(fits & (col_b % 8 >= 4), take, 0.0).astype(BF16)

    len_out[...] = jnp.zeros((1, 128), I32)
    len_out[0:1, 0:8] = seen_ref[...]
    len_in[0] = len_out[...]
    back[0] = jnp.zeros((8, 128), BF16)

    def weights(s):
        return jnp.exp(50.0 * jnp.tanh(s * (1.0 / 600.0)))

    row16 = iota((16, 128), 0) // 2
    k_copy.wait()
    for t in range(8):
        s = jnp.zeros((16, 256), F32)
        for n in range(8):
            mine = jnp.where(row16 == n, q16.astype(F32), 0.0).astype(BF16)
            s = s + nt(mine, k_buf[table_s[n, t]])
        e_loc[t] = weights(s)

    pl.semaphore_wait(barrier, n_dp - 1 + n_heads - 1)

    def h_copy(k):
        return pltpu.make_async_remote_copy(
            src_ref=len_out, dst_ref=len_in.at[n_heads - k],
            send_sem=h_send.at[k], recv_sem=h_recv.at[n_heads - k],
            device_id={"heads": across(k)}, device_id_type=MESH,
        )

    def dp_copy(src_ref, dst, send, recv, o):
        return pltpu.make_async_remote_copy(
            src_ref=src_ref, dst_ref=dst.at[opposite(o)],
            send_sem=send.at[o], recv_sem=recv.at[opposite(o)],
            device_id={"dp": peer(o)}, device_id_type=MESH,
        )

    def q_copy(o):
        return dp_copy(ask_q.at[o], got_q, q_send, q_recv, o)

    def w_copy(o):
        return dp_copy(ask_w.at[o], got_w, w_send, w_recv, o)

    def l_copy(o):
        return dp_copy(len_max, got_len, l_send, l_recv, o)

    def b_copy(o):
        return dp_copy(give.at[o], back, b_send, b_recv, o)

    for k in range(1, n_heads):
        h_copy(k).start()
    for o in FAR_FIRST:
        w_copy(o).start()
        q_copy(o).start()
    for k in range(1, n_heads):
        h_copy(n_heads - k).wait_recv()
    lengths = jnp.max(len_in[...], axis=0)
    len_max[...] = lengths
    for o in FAR_FIRST:
        l_copy(o).start()

    lens_f = lengths.astype(F32)
    r16, l16 = iota((16, 128), 0) // 2, iota((16, 128), 1)
    len_col = jnp.sum(jnp.where(r16 == l16, lens_f, 0.0), axis=1, keepdims=True)
    tok16 = iota((16, 256), 1).astype(F32)
    row16w = iota((16, 256), 0) // 2
    went = jnp.zeros((8, 8), F32)
    ent_row = entry
    hot8 = jnp.where((iota((16, rows), 0) // 2).astype(F32) == session, 1.0, 0.0)
    num = jnp.zeros((16, 128), F32)
    den = jnp.zeros((16, 256), F32)
    v_copy.wait()
    for t in range(8):
        moved = jnp.sum(jnp.where(page == float(t), hot8, 0.0), axis=1, keepdims=True)
        limit = jnp.where(moved > 0.0, 0.0, len_col - 256.0 * t)
        w = jnp.where(tok16 < limit, e_loc[t], 0.0).astype(BF16).astype(F32)
        den = den + w
        for n in range(8):
            mine = jnp.where(row16w == n, w, 0.0).astype(BF16)
            num = num + nn(mine, v_buf[table_s[n, t]])
    den = jnp.sum(den, axis=1, keepdims=True)

    row8 = iota((8, 128), 0)
    slots = {}
    for o in NEAR_FIRST:
        w_copy(opposite(o)).wait_recv()
        q_copy(opposite(o)).wait_recv()
        q8 = got_q[o].astype(F32)
        words_o = got_w[o]
        a, b = words_o[0, 0], words_o[0, 1]
        slots[o] = (a, b)
        s = nt(jnp.where(row8 < 2, q8, 0.0).astype(BF16), k_buf[a % 64])
        s = s + nt(jnp.where(row8 >= 2, q8, 0.0).astype(BF16), k_buf[b % 64])
        e_far[o] = weights(s)
    lane8 = iota((8, 128), 1)
    tok8, row8w = iota((8, 256), 1).astype(F32), iota((8, 256), 0)
    first = iota((8, 1), 0) < 2
    for o in NEAR_FIRST:
        a, b = slots[o]
        l_copy(opposite(o)).wait_recv()
        who = jnp.where(row8 < 2, a // 64 % 8, b // 64 % 8)
        part = jnp.where(first, a // 512 * 256, b // 512 * 256).astype(F32)
        length = jnp.sum(jnp.where(lane8 == who, got_len[o].astype(F32), 0.0), axis=1, keepdims=True)
        w = jnp.where(tok8 < length - part, e_far[o], 0.0).astype(BF16).astype(F32)
        d = jnp.sum(w, axis=1, keepdims=True)
        m = nn(jnp.where(row8w < 2, w, 0.0).astype(BF16), v_buf[a % 64])
        m = m + nn(jnp.where(row8w >= 2, w, 0.0).astype(BF16), v_buf[b % 64])
        d = jnp.broadcast_to(d, (8, 128))
        d = pltpu.roll(d, 4, 0)
        give[o] = jnp.where(row8 < 4, m, d).astype(BF16)
        b_copy(o).start()

    for o in NEAR_FIRST:
        b_copy(opposite(o)).wait_recv()
    got = back[...].astype(F32).reshape(n_back, 128).astype(BF16)
    num = num + nn(take_num, got)
    den = den + nn(take_den, got)
    live = jnp.sum(jnp.where(r16 == l16, fin16(fin_ref), 0.0), axis=1, keepdims=True)
    out_ref[...] = jnp.where(live == 1.0, 0.0, num / den).astype(BF16)

    for k in range(1, n_heads):
        h_copy(k).wait_send()
    for o in FAR_FIRST:
        w_copy(o).wait_send()
        q_copy(o).wait_send()
        l_copy(o).wait_send()
        b_copy(o).wait_send()


def fin16(fin_ref):
    row = fin_ref[...].astype(F32)
    return jnp.concatenate([row, jnp.zeros((1, 128 - row.shape[1]), F32)], axis=1)


def body(queries, key_cache, value_cache, lengths_seen, page_table, finished, move_plan):
    n_dp, n_heads = lax.axis_size("dp"), lax.axis_size("heads")
    slots, _, page, dim = key_cache.shape
    sessions, group, _ = queries.shape
    vmem = pl.BlockSpec(memory_space=pltpu.VMEM)
    hbm = pl.BlockSpec(memory_space=pl.ANY)
    dma = pltpu.SemaphoreType.DMA
    out = pl.pallas_call(
        functools.partial(kernel, n_dp, n_heads),
        out_shape=jax.ShapeDtypeStruct((sessions * group, dim), BF16),
        in_specs=[pl.BlockSpec(memory_space=pltpu.SMEM), vmem, hbm, hbm, vmem, vmem, vmem, vmem],
        out_specs=vmem,
        scratch_shapes=[
            pltpu.VMEM((slots, page, dim), BF16),
            pltpu.VMEM((slots, page, dim), BF16),
            pltpu.VMEM((n_dp, 8, dim), BF16),
            pltpu.VMEM((n_dp, 1, 128), I32),
            pltpu.VMEM((n_dp, 8, dim), BF16),
            pltpu.VMEM((n_dp, 1, 128), I32),
            pltpu.VMEM((1, 128), I32),
            pltpu.VMEM((n_heads, 1, 128), I32),
            pltpu.VMEM((1, 128), I32),
            pltpu.VMEM((n_dp, 1, 128), I32),
            pltpu.VMEM((8, 16, page), F32),
            pltpu.VMEM((n_dp, 8, page), F32),
            pltpu.VMEM((n_dp, 8, dim), BF16),
            pltpu.VMEM((n_dp, 8, dim), BF16),
            dma((2,)),
            dma((n_heads,)), dma((n_heads + 1,)),
            dma((n_dp,)), dma((n_dp,)),
            dma((n_dp,)), dma((n_dp,)),
            dma((n_dp,)), dma((n_dp,)),
            dma((n_dp,)), dma((n_dp,)),
        ],
        compiler_params=pltpu.CompilerParams(
            collective_id=0, has_side_effects=True, vmem_limit_bytes=48 << 20
        ),
        name="attend",
    )(
        page_table,
        queries,
        key_cache.reshape(slots, page, dim),
        value_cache.reshape(slots, page, dim),
        lengths_seen.reshape(1, sessions),
        page_table,
        finished.reshape(1, sessions),
        move_plan.T,
    )
    return out.reshape(sessions, group, dim)


def solution(mesh):
    in_specs = (
        P("dp", "heads", None),
        P("dp", "heads", None, None),
        P("dp", "heads", None, None),
        P("dp", "heads"),
        P("dp", None),
        P("dp"),
        P("dp", None),
    )
    out_specs = P("dp", "heads", None)
    return jax.shard_map(body, mesh=mesh, in_specs=in_specs, out_specs=out_specs, check_vma=False)
```

```python
import functools

import jax
import jax.numpy as jnp
from jax import lax
from jax.experimental import pallas as pl
from jax.experimental.pallas import tpu as pltpu
from jax.sharding import PartitionSpec as P

MESH = pl.DeviceIdType.MESH
F32, BF16, I32 = jnp.float32, jnp.bfloat16, jnp.int32
BATCH = 4


def nt(a, b, precision=None):
    return lax.dot_general(
        a, b, (((1,), (1,)), ((), ())), precision=precision, preferred_element_type=F32
    )


def nn(a, b, precision=None):
    return lax.dot_general(
        a, b, (((1,), (0,)), ((), ())), precision=precision, preferred_element_type=F32
    )


def iota(shape, dim):
    return lax.broadcasted_iota(I32, shape, dim)


def one_hot(mask):
    return jnp.where(mask, 1.0, 0.0).astype(BF16)


def weights(s):
    return jnp.exp(50.0 * jnp.tanh(s * (1.0 / 600.0)))


def kernel(
    n_dp, n_heads,
    q_hbm, k_hbm, v_hbm, seen_hbm, table_hbm, fin_hbm, plan_hbm,
    out_ref,
    q_ref, k_buf, v_buf, seen_ref, table_s, table_ref, fin_ref, plan_ref,
    ask_q, ask_w, got_q, got_w, len_out, len_in, e_loc, give, back,
    in_sem, kv_sem, in_dp, in_h, h_send, h_recv, q_send, q_recv, w_send, w_recv, b_send, b_recv,
):
    me, head = lax.axis_index("dp"), lax.axis_index("heads")

    barrier = pltpu.get_barrier_semaphore()

    @pl.loop(me + 1, n_dp)
    def _(d):
        pl.semaphore_signal(barrier, inc=1, device_id={"dp": d}, device_id_type=MESH)

    @pl.loop(head + 1, n_heads)
    def _(h):
        pl.semaphore_signal(barrier, inc=1, device_id={"heads": h}, device_id_type=MESH)

    small = [
        pltpu.make_async_copy(src, dst, in_sem.at[i])
        for i, (src, dst) in enumerate(
            [(seen_hbm, seen_ref), (plan_hbm, plan_ref), (table_hbm, table_ref),
             (q_hbm, q_ref), (table_hbm, table_s), (fin_hbm, fin_ref)]
        )
    ]
    for c in small:
        c.start()
    k_copy = pltpu.make_async_copy(k_hbm, k_buf, kv_sem.at[0])
    v_copy = pltpu.make_async_copy(v_hbm, v_buf, kv_sem.at[1])
    k_copy.start()
    v_copy.start()

    @pl.when(me + head > 0)
    def _():
        pl.semaphore_wait(barrier, me + head)

    @pl.loop(0, me)
    def _(d):
        pl.semaphore_signal(in_dp.at[me], inc=1, device_id={"dp": d}, device_id_type=MESH)

    @pl.loop(0, head)
    def _(h):
        pl.semaphore_signal(in_h.at[head], inc=1, device_id={"heads": h}, device_id_type=MESH)

    def h_copy(h):
        return pltpu.make_async_remote_copy(
            src_ref=len_out, dst_ref=len_in.at[head],
            send_sem=h_send.at[h], recv_sem=h_recv.at[head],
            device_id={"heads": h}, device_id_type=MESH,
        )

    def h_arrival(h):
        return pltpu.make_async_remote_copy(
            src_ref=len_out, dst_ref=len_in.at[h],
            send_sem=h_send.at[h], recv_sem=h_recv.at[h],
            device_id={"heads": h}, device_id_type=MESH,
        )

    for c in small:
        c.wait()
    len_out[...] = jnp.zeros((1, 128), I32)
    len_out[0:1, 0:8] = seen_ref[...]
    len_in[head] = len_out[...]

    @pl.loop(0, n_heads)
    def _(h):
        @pl.when(h > head)
        def _():
            pl.semaphore_wait(in_h.at[h], 1)

        @pl.when(h != head)
        def _():
            h_copy(h).start()

    src, slot, dest = plan_ref[0:1, :].astype(F32), plan_ref[1:2, :].astype(F32), plan_ref[2:3, :]
    rows = src.shape[1]
    sub, lane = iota((rows, rows), 0), iota((rows, rows), 1)
    src_col = jnp.sum(jnp.where(sub == lane, src, 0.0), axis=1, keepdims=True)
    same = (src_col == src) & (sub < lane)
    rank = jnp.sum(jnp.where(same, 1.0, 0.0), axis=0, keepdims=True)
    place = src * 2.0 + rank
    sub8 = iota((8, rows), 0)
    entry = jnp.zeros((8, rows), F32)
    for t in range(8):
        hit = table_ref[:, t : t + 1] == dest
        entry = entry + jnp.where(hit, (sub8 * 8 + t).astype(F32), 0.0)
    entry = jnp.sum(entry, axis=0, keepdims=True)
    session = jnp.floor(entry * 0.125)
    page = entry - session * 8.0

    row16 = iota((16, rows), 0) // 2
    hot16f = jnp.where(row16.astype(F32) == session, 1.0, 0.0)
    hot16 = hot16f.astype(BF16)
    n_back = n_dp * 8
    r8 = iota((n_back, rows), 0)
    spread = one_hot((r8 // 8 * 2 + (r8 % 8 // 2) % 2).astype(F32) == place)
    pick = nt(spread, hot16)
    row_a, col_a = iota((n_back, 16), 0), iota((n_back, 16), 1)
    pick = jnp.where((row_a % 2 == col_a % 2) & (row_a % 8 < 4), pick, 0.0).astype(BF16)
    q16 = q_ref[...].astype(F32).reshape(16, 128).astype(BF16)
    ask_q[...] = nn(pick, q16).reshape(n_dp, 8, 128).astype(BF16)
    at = one_hot(iota((n_dp, rows), 0).astype(F32) == src)
    mine_w = iota((128, rows), 0).astype(F32) == rank
    slot_part = nt(at, jnp.where(mine_w, slot, 0.0).astype(BF16))

    take = nt(hot16, spread)
    row_b, col_b = iota((16, n_back), 0), iota((16, n_back), 1)
    fits = row_b % 2 == col_b % 2
    take_num = jnp.where(fits & (col_b % 8 < 4), take, 0.0).astype(BF16)
    take_den = jnp.where(fits & (col_b % 8 >= 4), take, 0.0).astype(BF16)
    back[me] = jnp.zeros((8, 128), BF16)
    moved = [
        jnp.sum(jnp.where(page == float(t), hot16f, 0.0), axis=1, keepdims=True) for t in range(8)
    ]

    @pl.loop(0, n_heads)
    def _(h):
        @pl.when(h != head)
        def _():
            h_arrival(h).wait_recv()

    lengths = jnp.max(len_in[...], axis=0).astype(F32)
    r16, l16 = iota((16, 128), 0) // 2, iota((16, 128), 1)
    len_col = jnp.sum(jnp.where(r16 == l16, lengths, 0.0), axis=1, keepdims=True)
    row_len = jnp.sum(hot16f * len_col, axis=0, keepdims=True) * 0.5
    live = jnp.clip(row_len - 256.0 * page, 0.0, 256.0)
    live_part = nt(at, jnp.where(mine_w, live, 0.0).astype(BF16))
    ask_w[...] = (slot_part + 64.0 * live_part).astype(I32).reshape(n_dp, 1, 128)

    def q_copy(d, slot_at):
        return pltpu.make_async_remote_copy(
            src_ref=ask_q.at[d], dst_ref=got_q.at[slot_at],
            send_sem=q_send.at[d], recv_sem=q_recv.at[slot_at],
            device_id={"dp": d}, device_id_type=MESH,
        )

    def w_copy(d, slot_at):
        return pltpu.make_async_remote_copy(
            src_ref=ask_w.at[d], dst_ref=got_w.at[slot_at],
            send_sem=w_send.at[d], recv_sem=w_recv.at[slot_at],
            device_id={"dp": d}, device_id_type=MESH,
        )

    def b_copy(d, slot_at):
        return pltpu.make_async_remote_copy(
            src_ref=give.at[d], dst_ref=back.at[slot_at],
            send_sem=b_send.at[d], recv_sem=b_recv.at[slot_at],
            device_id={"dp": d}, device_id_type=MESH,
        )

    @pl.loop(0, n_dp)
    def _(d):
        @pl.when(d > me)
        def _():
            pl.semaphore_wait(in_dp.at[d], 1)

        @pl.when(d != me)
        def _():
            w_copy(d, me).start()
            q_copy(d, me).start()

    got_q[me] = jnp.zeros((8, 128), BF16)
    got_w[me] = jnp.zeros((1, 128), I32)

    row_q = iota((16, 128), 0) // 2
    k_copy.wait()
    q16f = q16.astype(F32)
    for t in range(8):
        s = jnp.zeros((16, 256), F32)
        for n in range(8):
            s = s + nt(jnp.where(row_q == n, q16f, 0.0).astype(BF16), k_buf[table_s[n, t]])
        e_loc[t] = weights(s)
    tok16 = iota((16, 256), 1).astype(F32)
    row_w = iota((16, 256), 0) // 2
    num = jnp.zeros((16, 128), F32)
    den = jnp.zeros((16, 256), F32)
    v_copy.wait()
    for t in range(8):
        limit = jnp.where(moved[t] > 0.0, 0.0, len_col - 256.0 * t)
        w = jnp.where(tok16 < limit, e_loc[t], 0.0).astype(BF16).astype(F32)
        den = den + w
        for n in range(8):
            num = num + nn(jnp.where(row_w == n, w, 0.0).astype(BF16), v_buf[table_s[n, t]])
    den = jnp.sum(den, axis=1, keepdims=True)

    row8, row8w = iota((8, 128), 0), iota((8, 256), 0)
    tok8 = iota((8, 256), 1)

    @pl.loop(0, n_dp // BATCH)
    def _(i):
        held = []
        for j in range(BATCH):
            d = i * BATCH + j

            @pl.when(d != me)
            def _():
                w_copy(d, d).wait_recv()
                q_copy(d, d).wait_recv()

        for j in range(BATCH):
            d = i * BATCH + j
            q8 = got_q[d].astype(F32)
            words = got_w[d]
            a, b = words[0, 0], words[0, 1]
            s = nt(jnp.where(row8 < 2, q8, 0.0).astype(BF16), k_buf[a & 63])
            s = s + nt(jnp.where(row8 >= 2, q8, 0.0).astype(BF16), k_buf[b & 63])
            held.append((d, a, b, s))
        for d, a, b, s in held:
            limit = jnp.where(row8w < 2, a >> 6, b >> 6)
            w = jnp.where(tok8 < limit, weights(s), 0.0).astype(BF16).astype(F32)
            m = nn(jnp.where(row8w < 2, w, 0.0).astype(BF16), v_buf[a & 63])
            m = m + nn(jnp.where(row8w >= 2, w, 0.0).astype(BF16), v_buf[b & 63])
            total = jnp.broadcast_to(jnp.sum(w, axis=1, keepdims=True), (8, 128))
            give[d] = jnp.where(row8 < 4, m, pltpu.roll(total, 4, 0)).astype(BF16)
        for j in range(BATCH):
            d = i * BATCH + j

            @pl.when(d != me)
            def _():
                b_copy(d, me).start()

    @pl.loop(0, n_dp)
    def _(d):
        @pl.when(d != me)
        def _():
            b_copy(d, d).wait_recv()

    got = back[...].astype(F32).reshape(n_back, 128).astype(BF16)
    num = num + nn(take_num, got)
    den = den + nn(take_den, got)
    ended = jnp.concatenate([fin_ref[...].astype(F32), jnp.zeros((1, 120), F32)], axis=1)
    ended = jnp.sum(jnp.where(r16 == l16, ended, 0.0), axis=1, keepdims=True)
    out_ref[...] = jnp.where(ended == 1.0, 0.0, num / den).astype(BF16)

    @pl.loop(0, n_heads)
    def _(h):
        @pl.when(h != head)
        def _():
            h_copy(h).wait_send()

    @pl.loop(0, n_dp)
    def _(d):
        @pl.when(d != me)
        def _():
            w_copy(d, me).wait_send()
            q_copy(d, me).wait_send()
            b_copy(d, me).wait_send()


def body(queries, key_cache, value_cache, lengths_seen, page_table, finished, move_plan):
    n_dp, n_heads = lax.axis_size("dp"), lax.axis_size("heads")
    slots, _, page, dim = key_cache.shape
    sessions, group, _ = queries.shape
    moves = move_plan.shape[0]
    hbm = pl.BlockSpec(memory_space=pltpu.HBM)
    dma, regular = pltpu.SemaphoreType.DMA, pltpu.SemaphoreType.REGULAR
    vmem = pltpu.VMEM
    out = pl.pallas_call(
        functools.partial(kernel, n_dp, n_heads),
        out_shape=jax.ShapeDtypeStruct((sessions * group, dim), BF16),
        in_specs=[hbm] * 7,
        out_specs=pl.BlockSpec(memory_space=pltpu.VMEM),
        scratch_shapes=[
            vmem((sessions, group, dim), BF16),
            vmem((slots, page, dim), BF16),
            vmem((slots, page, dim), BF16),
            vmem((1, sessions), I32),
            pltpu.SMEM(page_table.shape, I32),
            vmem(page_table.shape, I32),
            vmem((1, sessions), I32),
            vmem((3, moves), I32),
            vmem((n_dp, 8, dim), BF16),
            vmem((n_dp, 1, 128), I32),
            vmem((n_dp, 8, dim), BF16),
            vmem((n_dp, 1, 128), I32),
            vmem((1, 128), I32),
            vmem((n_heads, 1, 128), I32),
            vmem((8, 16, page), F32),
            vmem((n_dp, 8, dim), BF16),
            vmem((n_dp, 8, dim), BF16),
            dma((6,)), dma((2,)),
            regular((n_dp,)), regular((n_heads,)),
            dma((n_heads,)), dma((n_heads,)),
            dma((n_dp,)), dma((n_dp,)),
            dma((n_dp,)), dma((n_dp,)),
            dma((n_dp,)), dma((n_dp,)),
        ],
        compiler_params=pltpu.CompilerParams(
            collective_id=0, has_side_effects=True, vmem_limit_bytes=67043328
        ),
        name="attend",
    )(
        queries,
        key_cache.reshape(slots, page, dim),
        value_cache.reshape(slots, page, dim),
        lengths_seen.reshape(1, sessions),
        page_table,
        finished.reshape(1, sessions),
        move_plan.T,
    )
    return out.reshape(sessions, group, dim)


def solution(mesh):
    in_specs = (
        P("dp", "heads", None),
        P("dp", "heads", None, None),
        P("dp", "heads", None, None),
        P("dp", "heads"),
        P("dp", None),
        P("dp"),
        P("dp", None),
    )
    out_specs = P("dp", "heads", None)
    return jax.shard_map(body, mesh=mesh, in_specs=in_specs, out_specs=out_specs, check_vma=False)
```

```python
import functools

import jax
import jax.numpy as jnp
from jax import lax
from jax.experimental import pallas as pl
from jax.experimental.pallas import tpu as pltpu
from jax.sharding import PartitionSpec as P

MESH = pl.DeviceIdType.MESH
F32, BF16, I32 = jnp.float32, jnp.bfloat16, jnp.int32
NZ, NX = 8, 4


def nt(a, b, precision=None):
    return lax.dot_general(
        a, b, (((1,), (1,)), ((), ())), precision=precision, preferred_element_type=F32
    )


def nn(a, b, precision=None):
    return lax.dot_general(
        a, b, (((1,), (0,)), ((), ())), precision=precision, preferred_element_type=F32
    )


def iota(shape, dim):
    return lax.broadcasted_iota(I32, shape, dim)


def swap(h):
    return h + 1 - 2 * (h % 2)


def one_hot(mask):
    return jnp.where(mask, 1.0, 0.0).astype(BF16)


def weights(s):
    return jnp.exp(50.0 * jnp.tanh(s * (1.0 / 600.0)))


def kernel(
    n_dp, n_heads,
    q_hbm, k_hbm, v_hbm, seen_hbm, table_hbm, fin_hbm, plan_hbm,
    out_ref,
    q_ref, k_buf, v_buf, seen_ref, table_s, table_ref, fin_ref, plan_ref,
    ask_q, ask_w, mid_q, mid_w, got_q, got_w, len_out, len_in, e_loc, give, back,
    in_sem, kv_sem, in_z, in_x, in_h, in_all, h_send, h_recv,
    xq_send, xq_recv, xw_send, xw_recv, zq_send, zq_recv, zw_send, zw_recv, b_send, b_recv,
):
    me, head = lax.axis_index("dp"), lax.axis_index("heads")
    mz, mx = me // NX, me % NX

    def at_z(z):
        return {"dp": z * NX + mx}

    def at_x(x):
        return {"dp": mz * NX + x}

    half = NZ // 2
    early = mz < half
    rank_h = swap(head)

    barrier = pltpu.get_barrier_semaphore()

    @pl.when(early)
    def _():
        @pl.loop(mz + 1, NZ)
        def _(z):
            pl.semaphore_signal(barrier, inc=1, device_id=at_z(z), device_id_type=MESH)

    @pl.loop(mx + 1, NX)
    def _(x):
        pl.semaphore_signal(barrier, inc=1, device_id=at_x(x), device_id_type=MESH)

    @pl.loop(rank_h + 1, n_heads)
    def _(r):
        pl.semaphore_signal(barrier, inc=1, device_id={"heads": swap(r)}, device_id_type=MESH)

    small = [
        pltpu.make_async_copy(src, dst, in_sem.at[i])
        for i, (src, dst) in enumerate(
            [(seen_hbm, seen_ref), (plan_hbm, plan_ref), (table_hbm, table_ref),
             (q_hbm, q_ref), (table_hbm, table_s), (fin_hbm, fin_ref)]
        )
    ]
    for c in small:
        c.start()
    k_copy = pltpu.make_async_copy(k_hbm, k_buf, kv_sem.at[0])
    v_copy = pltpu.make_async_copy(v_hbm, v_buf, kv_sem.at[1])
    k_copy.start()
    v_copy.start()

    before = jnp.where(early, mz, half)

    @pl.when(before + mx + rank_h > 0)
    def _():
        pl.semaphore_wait(barrier, before + mx + rank_h)

    @pl.loop(0, before)
    def _(z):
        pl.semaphore_signal(in_z.at[mz], inc=1, device_id=at_z(z), device_id_type=MESH)

    @pl.loop(0, rank_h)
    def _(r):
        pl.semaphore_signal(in_h.at[head], inc=1, device_id={"heads": swap(r)}, device_id_type=MESH)

    @pl.loop(0, mx)
    def _(x):
        pl.semaphore_signal(in_x.at[mx], inc=1, device_id=at_x(x), device_id_type=MESH)

    def h_copy(h):
        return pltpu.make_async_remote_copy(
            src_ref=len_out, dst_ref=len_in.at[head],
            send_sem=h_send.at[h], recv_sem=h_recv.at[head],
            device_id={"heads": h}, device_id_type=MESH,
        )

    def h_arrival(h):
        return pltpu.make_async_remote_copy(
            src_ref=len_out, dst_ref=len_in.at[h],
            send_sem=h_send.at[h], recv_sem=h_recv.at[h],
            device_id={"heads": h}, device_id_type=MESH,
        )

    small[0].wait()
    len_out[...] = jnp.zeros((1, 128), I32)
    len_out[0:1, 0:8] = seen_ref[...]
    len_in[head] = len_out[...]

    @pl.loop(0, n_heads)
    def _(r):
        h = swap(r)

        @pl.when(r > rank_h)
        def _():
            pl.semaphore_wait(in_h.at[h], 1)

        @pl.when(r != rank_h)
        def _():
            h_copy(h).start()

    for c in small[1:]:
        c.wait()

    def x_copy(src, dst, send, recv, x, x_from):
        return pltpu.make_async_remote_copy(
            src_ref=src.at[x], dst_ref=dst.at[x_from], send_sem=send.at[x], recv_sem=recv.at[x_from],
            device_id=at_x(x), device_id_type=MESH,
        )

    def z_copy(src, dst, send, recv, z, z_from):
        return pltpu.make_async_remote_copy(
            src_ref=src.at[:, z], dst_ref=dst.at[z_from], send_sem=send.at[z], recv_sem=recv.at[z_from],
            device_id=at_z(z), device_id_type=MESH,
        )

    def xq_copy(x, x_from):
        return x_copy(ask_q, mid_q, xq_send, xq_recv, x, x_from)

    def xw_copy(x, x_from):
        return x_copy(ask_w, mid_w, xw_send, xw_recv, x, x_from)

    def zq_copy(z, z_from):
        return z_copy(mid_q, got_q, zq_send, zq_recv, z, z_from)

    def zw_copy(z, z_from):
        return z_copy(mid_w, got_w, zw_send, zw_recv, z, z_from)

    def b_copy(d, place_at):
        return pltpu.make_async_remote_copy(
            src_ref=give.at[d], dst_ref=back.at[place_at], send_sem=b_send.at[d], recv_sem=b_recv.at[place_at],
            device_id={"dp": d}, device_id_type=MESH,
        )

    src, slot, dest = plan_ref[0:1, :].astype(F32), plan_ref[1:2, :].astype(F32), plan_ref[2:3, :]
    rows = src.shape[1]
    src_z = jnp.floor(src / NX)
    src = (src - NX * src_z) * NZ + src_z
    sub, lane = iota((rows, rows), 0), iota((rows, rows), 1)
    src_col = jnp.sum(jnp.where(sub == lane, src, 0.0), axis=1, keepdims=True)
    same = (src_col == src) & (sub < lane)
    rank = jnp.sum(jnp.where(same, 1.0, 0.0), axis=0, keepdims=True)
    place = src * 2.0 + rank
    sub8 = iota((8, rows), 0)
    entry = jnp.zeros((8, rows), F32)
    for t in range(8):
        hit = table_ref[:, t : t + 1] == dest
        entry = entry + jnp.where(hit, (sub8 * 8 + t).astype(F32), 0.0)
    entry = jnp.sum(entry, axis=0, keepdims=True)
    session = jnp.floor(entry * 0.125)
    page = entry - session * 8.0

    row16 = iota((16, rows), 0) // 2
    hot16f = jnp.where(row16.astype(F32) == session, 1.0, 0.0)
    hot16 = hot16f.astype(BF16)
    n_back = n_dp * 8
    r8 = iota((n_back, rows), 0)
    spread = one_hot((r8 // 8 * 2 + (r8 % 8 // 2) % 2).astype(F32) == place)
    pick = nt(spread, hot16)
    row_a, col_a = iota((n_back, 16), 0), iota((n_back, 16), 1)
    pick = jnp.where((row_a % 2 == col_a % 2) & (row_a % 8 < 4), pick, 0.0).astype(BF16)
    q16 = q_ref[...].astype(F32).reshape(16, 128).astype(BF16)
    ask_q[...] = nn(pick, q16).reshape(NX, NZ, 8, 128).astype(BF16)
    mid_q[mx] = ask_q[mx]

    @pl.loop(0, NX)
    def _(x):
        @pl.when(x > mx)
        def _():
            pl.semaphore_wait(in_x.at[x], 1)

        @pl.when(x != mx)
        def _():
            xq_copy(x, mx).start()

    at = one_hot(iota((n_dp, rows), 0).astype(F32) == src)
    mine_w = iota((128, rows), 0).astype(F32) == rank
    slot_part = nt(at, jnp.where(mine_w, slot, 0.0).astype(BF16))

    take = nt(hot16, spread)
    row_b, col_b = iota((16, n_back), 0), iota((16, n_back), 1)
    fits = row_b % 2 == col_b % 2
    take_num = jnp.where(fits & (col_b % 8 < 4), take, 0.0).astype(BF16)
    take_den = jnp.where(fits & (col_b % 8 >= 4), take, 0.0).astype(BF16)
    back[mx * NZ + mz] = jnp.zeros((8, 128), BF16)
    moved = [
        jnp.sum(jnp.where(page == float(t), hot16f, 0.0), axis=1, keepdims=True) for t in range(8)
    ]

    @pl.loop(0, n_heads)
    def _(h):
        @pl.when(h != head)
        def _():
            h_arrival(h).wait_recv()

    lengths = jnp.max(len_in[...], axis=0).astype(F32)
    r16, l16 = iota((16, 128), 0) // 2, iota((16, 128), 1)
    len_col = jnp.sum(jnp.where(r16 == l16, lengths, 0.0), axis=1, keepdims=True)
    row_len = jnp.sum(hot16f * len_col, axis=0, keepdims=True) * 0.5
    live = jnp.clip(row_len - 256.0 * page, 0.0, 256.0)
    live_part = nt(at, jnp.where(mine_w, live, 0.0).astype(BF16))
    ask_w[...] = (slot_part + 64.0 * live_part).astype(I32).reshape(NX, NZ, 1, 128)

    mid_w[mx] = ask_w[mx]

    @pl.loop(0, NX)
    def _(x):
        @pl.when(x != mx)
        def _():
            xw_copy(x, mx).start()

    row_q = iota((16, 128), 0) // 2
    k_copy.wait()
    q16f = q16.astype(F32)
    for t in range(8):
        s = jnp.zeros((16, 256), F32)
        for n in range(8):
            s = s + nt(jnp.where(row_q == n, q16f, 0.0).astype(BF16), k_buf[table_s[n, t]])
        e_loc[t] = weights(s)
    tok16 = iota((16, 256), 1).astype(F32)
    row_w = iota((16, 256), 0) // 2
    num = jnp.zeros((16, 128), F32)
    den = jnp.zeros((16, 256), F32)
    v_copy.wait()
    for t in range(8):
        limit = jnp.where(moved[t] > 0.0, 0.0, len_col - 256.0 * t)
        w = jnp.where(tok16 < limit, e_loc[t], 0.0).astype(BF16).astype(F32)
        den = den + w
        for n in range(8):
            num = num + nn(jnp.where(row_w == n, w, 0.0).astype(BF16), v_buf[table_s[n, t]])
    den = jnp.sum(den, axis=1, keepdims=True)

    @pl.loop(0, NX)
    def _(x):
        @pl.when(x != mx)
        def _():
            xq_copy(x, x).wait_recv()
            xw_copy(x, x).wait_recv()

    @pl.loop(0, NZ)
    def _(z):
        @pl.when(early & (z > mz))
        def _():
            pl.semaphore_wait(in_z.at[z], 1)

        @pl.when((mz >= half) & (z == half))
        def _():
            pl.semaphore_wait(in_all, 1)

        @pl.when(z != mz)
        def _():
            zw_copy(z, mz).start()
            zq_copy(z, mz).start()

    @pl.when(early)
    def _():
        pl.semaphore_signal(in_all, inc=1, device_id=at_z(NZ - 1 - mz), device_id_type=MESH)

    for x in range(NX):
        got_q[mz, x] = mid_q[x, mz]
        got_w[mz, x] = mid_w[x, mz]

    row8, row8w = iota((8, 128), 0), iota((8, 256), 0)
    tok8 = iota((8, 256), 1)

    @pl.loop(0, NZ)
    def _(z):
        @pl.when(z != mz)
        def _():
            zw_copy(z, z).wait_recv()
            zq_copy(z, z).wait_recv()

        held = []
        for x in range(NX):
            q8 = got_q[z, x].astype(F32)
            words = got_w[z, x]
            a, b = words[0, 0], words[0, 1]
            s = nt(jnp.where(row8 < 2, q8, 0.0).astype(BF16), k_buf[a & 63])
            s = s + nt(jnp.where(row8 >= 2, q8, 0.0).astype(BF16), k_buf[b & 63])
            held.append((z * NX + x, a, b, s))
        for d, a, b, s in held:
            limit = jnp.where(row8w < 2, a >> 6, b >> 6)
            w = jnp.where(tok8 < limit, weights(s), 0.0).astype(BF16).astype(F32)
            m = nn(jnp.where(row8w < 2, w, 0.0).astype(BF16), v_buf[a & 63])
            m = m + nn(jnp.where(row8w >= 2, w, 0.0).astype(BF16), v_buf[b & 63])
            total = jnp.broadcast_to(jnp.sum(w, axis=1, keepdims=True), (8, 128))
            give[d] = jnp.where(row8 < 4, m, pltpu.roll(total, 4, 0)).astype(BF16)
        for x in range(NX):
            d = z * NX + x

            @pl.when(d != me)
            def _():
                b_copy(d, mx * NZ + mz).start()

    @pl.loop(0, n_dp)
    def _(d):
        @pl.when(d != me)
        def _():
            b_copy(d, d % NX * NZ + d // NX).wait_recv()

    got = back[...].astype(F32).reshape(n_back, 128).astype(BF16)
    num = num + nn(take_num, got)
    den = den + nn(take_den, got)
    ended = jnp.concatenate([fin_ref[...].astype(F32), jnp.zeros((1, 120), F32)], axis=1)
    ended = jnp.sum(jnp.where(r16 == l16, ended, 0.0), axis=1, keepdims=True)
    out_ref[...] = jnp.where(ended == 1.0, 0.0, num / den).astype(BF16)

    @pl.loop(0, n_heads)
    def _(h):
        @pl.when(h != head)
        def _():
            h_copy(h).wait_send()

    @pl.loop(0, NX)
    def _(x):
        @pl.when(x != mx)
        def _():
            xq_copy(x, mx).wait_send()
            xw_copy(x, mx).wait_send()

    @pl.loop(0, NZ)
    def _(z):
        @pl.when(z != mz)
        def _():
            zq_copy(z, mz).wait_send()
            zw_copy(z, mz).wait_send()

    @pl.loop(0, n_dp)
    def _(d):
        @pl.when(d != me)
        def _():
            b_copy(d, me).wait_send()


def body(queries, key_cache, value_cache, lengths_seen, page_table, finished, move_plan):
    n_dp, n_heads = lax.axis_size("dp"), lax.axis_size("heads")
    slots, _, page, dim = key_cache.shape
    sessions, group, _ = queries.shape
    moves = move_plan.shape[0]
    hbm = pl.BlockSpec(memory_space=pltpu.HBM)
    dma, regular = pltpu.SemaphoreType.DMA, pltpu.SemaphoreType.REGULAR
    vmem = pltpu.VMEM
    out = pl.pallas_call(
        functools.partial(kernel, n_dp, n_heads),
        out_shape=vmem((sessions * group, dim), BF16),
        in_specs=[hbm] * 7,
        out_specs=pl.BlockSpec(memory_space=pltpu.VMEM),
        scratch_shapes=[
            vmem((sessions, group, dim), BF16),
            vmem((slots, page, dim), BF16),
            vmem((slots, page, dim), BF16),
            vmem((1, sessions), I32),
            pltpu.SMEM(page_table.shape, I32),
            vmem(page_table.shape, I32),
            vmem((1, sessions), I32),
            vmem((3, moves), I32),
            vmem((NX, NZ, 8, dim), BF16),
            vmem((NX, NZ, 1, 128), I32),
            vmem((NX, NZ, 8, dim), BF16),
            vmem((NX, NZ, 1, 128), I32),
            vmem((NZ, NX, 8, dim), BF16),
            vmem((NZ, NX, 1, 128), I32),
            vmem((1, 128), I32),
            vmem((n_heads, 1, 128), I32),
            vmem((8, 16, page), F32),
            vmem((n_dp, 8, dim), BF16),
            vmem((n_dp, 8, dim), BF16),
            dma((6,)), dma((2,)),
            regular((NZ,)), regular((NX,)), regular((n_heads,)), regular,
            dma((n_heads,)), dma((n_heads,)),
            dma((NX,)), dma((NX,)), dma((NX,)), dma((NX,)),
            dma((NZ,)), dma((NZ,)), dma((NZ,)), dma((NZ,)),
            dma((n_dp,)), dma((n_dp,)),
        ],
        compiler_params=pltpu.CompilerParams(
            collective_id=0, has_side_effects=True, vmem_limit_bytes=48 << 20
        ),
        name="attend",
    )(*[pltpu.with_memory_space_constraint(a, pltpu.HBM) for a in (
        queries,
        key_cache.reshape(slots, page, dim),
        value_cache.reshape(slots, page, dim),
        lengths_seen.reshape(1, sessions),
        page_table,
        finished.reshape(1, sessions),
        move_plan.T,
    )])
    return out.reshape(sessions, group, dim)


def solution(mesh):
    in_specs = (
        P("dp", "heads", None),
        P("dp", "heads", None, None),
        P("dp", "heads", None, None),
        P("dp", "heads"),
        P("dp", None),
        P("dp"),
        P("dp", None),
    )
    out_specs = P("dp", "heads", None)
    return jax.shard_map(body, mesh=mesh, in_specs=in_specs, out_specs=out_specs, check_vma=False)
```
